32 devices in a mesh: pairs: 16 (over z, y, x), comp: 2 (over core).
Axes of the slice: x: 2, y: 2, z: 4, core: 2. Of those that a mesh axis runs over, the one named last changes fastest.
Arguments:
- effects: float32 [49, 131072], P(None, 'pairs'), may hold values from -24 to 24
- se_table: float32 [16, 49], replicated, may hold values from 0.5 to 2
- se_index: int32 [256], P('pairs'), may hold values from 0 to 15
- base_root: float32 [16, 49, 49], replicated, may hold values from -0.875 to 0.875
- grid_scale: float32 [16], replicated, may hold values from 0.25 to 4
- comp_base: int32 [256], P('comp'), may hold values from 0 to 15
- comp_grid: int32 [256], P('comp'), may hold values from 0 to 15
- weights: float32 [256], P('comp'), may hold values from 0.2 to 5
Outputs:
- responsibility: float32 [256, 131072], P('comp', 'pairs')
- log_weights: float32 [256], P('comp')
- pair_loglik: float32 [131072], P('pairs')
The draws below stay inside these ranges and needn't reach their ends.
All inputs are finite; a program needn't handle non-finite values.
Results may differ from the reference program's by a relative error of at most 0.0003.
Values sent between devices are 32-bit elements; how exact they have to be, the bound alone decides.
A program may use at most 384 MiB of HBM per device.

```python
import math
import jax
import jax.numpy as jnp
from jax import lax

R = 49
NU = 16
NGRID = 16
NB = 16
TILE = 512
PAIRS = 131072
K = 256


def draw_effects(key, part):
    key_scale, key_base, key_flag, key_sign = jax.random.split(key, 4)
    values = 1.5 * jax.random.normal(key_base, (R, PAIRS), dtype=jnp.float32)
    return jnp.clip(values, -8.0, 8.0).astype(jnp.float32)


def plant(entries, rng, low, top_value):
    longest = entries.shape.index(max(entries.shape))
    spots = []
    for shift in (0, 1):
        where = [jax.random.randint(jax.random.fold_in(rng, axis), (), 0, length) for axis, length in enumerate(entries.shape)]
        where[longest] = (where[longest] + shift) % entries.shape[longest]
        spots.append(tuple(where))
    return entries.at[spots[0]].set(low).at[spots[1]].set(top_value)


def steps_of(stream_key, extent, pieces, least, top_value):
    gain, own = 1.0, jax.random.fold_in(stream_key, 6)
    for axis_at, blocks in pieces:
        heights = jnp.exp(jax.random.uniform(jax.random.fold_in(own, axis_at), (blocks,), jnp.float32, least / len(pieces), top_value / len(pieces)))
        gain = gain * jnp.repeat(heights, extent[axis_at] // blocks).reshape([-1 if axis == axis_at else 1 for axis in range(len(extent))])
    return gain


def normal_values(stream_key, shape, deviation, most, kind=jnp.bfloat16):
    return jnp.clip(deviation * jax.random.normal(stream_key, shape, jnp.float32), -most, most).astype(kind)


def setup_inputs(seed: int = 0) -> dict:
    arg_keys = jax.random.split(jax.random.key(seed), 9)
    return {
        "effects": draw_effects(jax.random.fold_in(arg_keys[8], 71), 0),
        "se_table": jnp.clip(jnp.exp(jax.random.uniform(arg_keys[1], (NB, R), jnp.float32, math.log(0.5), math.log(2.0))), 0.5, 2.0),
        "se_index": plant(jax.random.randint(arg_keys[2], (PAIRS // TILE,), 0, NB), jax.random.fold_in(arg_keys[2], 1), 0, NB - 1).astype(jnp.int32),
        "base_root": normal_values(arg_keys[3], (NU, R, R), R ** -0.5, 0.875, jnp.float32),
        "grid_scale": jnp.clip(jnp.exp(jax.random.uniform(arg_keys[4], (NGRID,), jnp.float32, math.log(0.25), math.log(4.0))), 0.25, 4.0),
        "comp_base": plant(jax.random.randint(arg_keys[5], (K,), 0, NU), jax.random.fold_in(arg_keys[5], 1), 0, NU - 1).astype(jnp.int32),
        "comp_grid": plant(jax.random.randint(arg_keys[6], (K,), 0, NGRID), jax.random.fold_in(arg_keys[6], 1), 0, NGRID - 1).astype(jnp.int32),
        "weights": jnp.clip(jnp.exp(math.log(5.0) - 3.218876 * jax.random.uniform(arg_keys[7], (K,), jnp.float32) ** steps_of(arg_keys[7], (K,), ((0, 2),), -0.2, 0.2)), 0.2, 5.0),
    }


def whiten_tables(se_table, base_root, grid_scale, comp_base, comp_grid):
    covariances = jnp.einsum('uij,ukj->uik', base_root, base_root, precision=lax.Precision.HIGHEST)
    picked = covariances[comp_base]
    scales = grid_scale[comp_grid]
    identity = jnp.eye(R, dtype=base_root.dtype)
    system = (scales * scales)[None, :, None, None] * picked[None]
    system = system + identity[None, None] * (se_table * se_table)[:, None, :, None]
    factor = jnp.linalg.cholesky(system)
    eye_full = jnp.broadcast_to(identity, factor.shape)
    inverse = jax.scipy.linalg.solve_triangular(factor, eye_full, lower=True)
    half_logdet = jnp.sum(jnp.log(jnp.diagonal(factor, axis1=2, axis2=3)), axis=-1)
    return (inverse, half_logdet)

def reference(effects, se_table, se_index, base_root, grid_scale, comp_base, comp_grid, weights):
    inverse, half_logdet = whiten_tables(se_table, base_root, grid_scale, comp_base, comp_grid)
    log_prior = jnp.log(weights)
    constant = 0.5 * R * math.log(2.0 * math.pi)
    tile_rows = effects.reshape(R, PAIRS // TILE, TILE).transpose(1, 0, 2)

    def one_tile(inputs):
        block_id, tile_data = inputs
        whitened = jnp.einsum('kij,jp->kip', inverse[block_id], tile_data, precision=lax.Precision.HIGHEST)
        quadratic = jnp.sum(whitened * whitened, axis=1)
        return log_prior[:, None] - 0.5 * quadratic - half_logdet[block_id][:, None] - constant
    scores = lax.map(one_tile, (se_index.astype(jnp.int32), tile_rows))
    scores = scores.transpose(1, 0, 2).reshape(K, PAIRS)
    score_max = jnp.max(scores, axis=0)
    score_sum = jnp.sum(jnp.exp(scores - score_max), axis=0)
    pair_loglik = score_max + jnp.log(score_sum)
    responsibility = jnp.exp(scores - pair_loglik)
    masses = jnp.sum(responsibility, axis=1)
    log_weights = jnp.log((masses + 1.0) / (PAIRS + K))
    return (responsibility, log_weights, pair_loglik)
```

```python
import math

import jax
import jax.numpy as jnp
from jax import lax
from jax.experimental import pallas as pl
from jax.experimental.pallas import tpu as pltpu
from jax.sharding import PartitionSpec as P

SUB = 8
GROUP = 4
MESH = pl.DeviceIdType.MESH


def split_terms(value):
    high = value.astype(jnp.bfloat16)
    return high, (value - high.astype(jnp.float32)).astype(jnp.bfloat16)


def put_row(table, row, inv):
    slot = table.shape[1] // 4
    comps = table.shape[2] // 2
    if len(inv) % 2:
        inv = inv + [jnp.zeros((SUB, comps), jnp.float32)]
    high, low = split_terms(jnp.concatenate(inv, axis=0))
    lanes = slice((row % 2) * comps, (row % 2 + 1) * comps)
    height = len(inv) * SUB
    table[row // 2, 0:height, lanes] = high
    table[row // 2, slot : slot + height, lanes] = high
    table[row // 2, 2 * slot : 2 * slot + height, lanes] = low
    table[row // 2, 3 * slot : 3 * slot + height, lanes] = low


def inverse_root(pivot):
    root = lax.rsqrt(pivot)
    return root * (1.5 - 0.5 * pivot * root * root)


def factor_steps(pattern, se_table, covar, prior, upper, inverse, edge, table, bias, tissues):
    constant = 0.5 * tissues * math.log(2.0 * math.pi)
    comps = covar.shape[2]
    border = tissues % SUB == 1
    core = tissues - 1 if border else tissues
    blocks = -(-core // SUB)
    sub_iota = lax.broadcasted_iota(jnp.int32, (SUB, comps), 0)
    half_logdet = jnp.zeros((1, comps), jnp.float32)
    for first in range(0, core, GROUP):
        row_block = first // SUB
        rows = range(first, min(first + GROUP, core))
        system, solved = {}, {}
        for row in rows:
            system[row] = [covar[row, v * SUB : (v + 1) * SUB, :] for v in range(row_block, blocks)]
            on_diag = sub_iota == row % SUB
            deviation = se_table[pattern, row]
            system[row][0] = system[row][0] + jnp.where(on_diag, deviation * deviation, 0.0)
            solved[row] = [jnp.zeros((SUB, comps), jnp.float32) for _ in range(row_block)]
            solved[row].append(jnp.where(on_diag, 1.0, 0.0))
        for col in range(first):
            col_block = col // SUB
            up = [upper[col, v * SUB : (v + 1) * SUB, :] for v in range(row_block, blocks)]
            inv = [inverse[col, v * SUB : (v + 1) * SUB, :] for v in range(col_block + 1)]
            for row in rows:
                mult = upper[col, row : row + 1, :]
                for n, part in enumerate(up):
                    system[row][n] = system[row][n] - mult * part
                for n, part in enumerate(inv):
                    solved[row][n] = solved[row][n] - mult * part
        for row in rows:
            pivot = system[row][0][row % SUB : row % SUB + 1, :]
            root = inverse_root(pivot)
            half_logdet = half_logdet + 0.5 * jnp.log(pivot)
            up = [part * root for part in system[row]]
            inv = [part * root for part in solved[row]]
            for n, part in enumerate(up):
                upper[row, (row_block + n) * SUB : (row_block + n + 1) * SUB, :] = part
            for n, part in enumerate(inv):
                inverse[row, n * SUB : (n + 1) * SUB, :] = part
            for later in rows:
                if later > row:
                    mult = up[0][later % SUB : later % SUB + 1, :]
                    for n, part in enumerate(up):
                        system[later][n] = system[later][n] - mult * part
                    for n, part in enumerate(inv):
                        solved[later][n] = solved[later][n] - mult * part
            put_row(table, row, inv)
            if border:
                terms = [part * covar[core, n * SUB : (n + 1) * SUB, :] for n, part in enumerate(inv)]
                edge[row : row + 1, :] = jnp.sum(sum(terms), axis=0, keepdims=True)
        yield
    if border:
        deviation = se_table[pattern, core]
        pivot = covar[core, core : core + 1, :] + deviation * deviation
        solved = [jnp.zeros((SUB, comps), jnp.float32) for _ in range(blocks)]
        for col in range(core):
            mult = edge[col : col + 1, :]
            pivot = pivot - mult * mult
            for n in range(col // SUB + 1):
                solved[n] = solved[n] - mult * inverse[col, n * SUB : (n + 1) * SUB, :]
        root = inverse_root(pivot)
        half_logdet = half_logdet + 0.5 * jnp.log(pivot)
        solved.append(jnp.where(sub_iota == core % SUB, 1.0, 0.0))
        put_row(table, core, [part * root for part in solved])
        yield
    bias[...] = jnp.log(prior[...]) - half_logdet - constant


def pack_tile(tile, effects, wide, ready):
    tissues = effects.shape[0]
    slot = wide.shape[0] // 2
    width = wide.shape[1]
    values = effects[:, pl.ds(pl.multiple_of(tile * width, width), width)]
    high = values.astype(jnp.bfloat16).astype(jnp.float32)
    wide[0:tissues, :] = high
    wide[slot : slot + tissues, :] = values - high
    ready[...] = wide[...].T.astype(jnp.bfloat16)


def finish_tile(tile, found, scaled, peak, total):
    width = found.shape[0]
    columns = pl.ds(pl.multiple_of(tile * width, width), width)
    values = found[...].T
    top = jnp.max(values, axis=0, keepdims=True)
    shifted = jnp.exp(values - top)
    scaled[:, columns] = shifted
    peak[:, columns] = top
    total[:, columns] = jnp.sum(shifted, axis=0, keepdims=True)


def score_steps(tissues, packed, table, bias, quad, found):
    comps = table.shape[2] // 2
    both = jnp.concatenate([packed[...], packed[...]], axis=1)
    last = table.shape[0] - 1
    for index in range(last + 1):
        if 2 * index + 1 < tissues:
            white = jnp.dot(both, table[index], preferred_element_type=jnp.float32)
            white = white * white
            part = white[:, :comps] + white[:, comps:]
        else:
            white = jnp.dot(both, table[index, :, :comps], preferred_element_type=jnp.float32)
            part = white * white
        if index == 0:
            quad[...] = part
        elif index < last:
            quad[...] += part
        else:
            found[...] = bias[...] - 0.5 * (quad[...] + part)
        if index % (GROUP // 2) == GROUP // 2 - 1:
            yield


def spread_covariances(roots, grid_scale, comp_base, comp_grid, stack, covar):
    tissues, bases = roots.shape[0], roots.shape[1]
    comps = covar.shape[2]
    for base in range(bases):
        root = roots[:, base, :]
        stack[:, base, :] = lax.dot_general(
            root, root, (((1,), (1,)), ((), ())),
            precision=lax.Precision.HIGHEST, preferred_element_type=jnp.float32,
        )
    pick = (lax.broadcasted_iota(jnp.int32, (bases, comps), 0) == comp_base[...]).astype(jnp.float32)
    pick = jnp.concatenate([pick, pick, pick], axis=0).astype(jnp.bfloat16)
    scale = jnp.zeros((1, comps), jnp.float32)
    for grid in range(grid_scale.shape[0]):
        scale = jnp.where(comp_grid[...] == grid, grid_scale[grid], scale)
    scale = scale * scale
    for row in range(tissues):
        value = stack[row]
        high = value.astype(jnp.bfloat16).astype(jnp.float32)
        rest = value - high
        middle = rest.astype(jnp.bfloat16).astype(jnp.float32)
        terms = jnp.concatenate([high, middle, rest - middle], axis=0).astype(jnp.bfloat16)
        spread = lax.dot_general(
            terms, pick, (((0,), (0,)), ((), ())), preferred_element_type=jnp.float32
        )
        covar[row, 0:tissues, :] = spread * scale


def score_body(se_index, se_table, grid_scale, effects, roots, comp_base, comp_grid, prior,
               scaled, peak, total,
               order, stack, covar, upper, inverse, edge, table, bias, quad, found, wide, packed, ready):
    tissues = effects.shape[0]
    tiles = se_index.shape[0]
    keys = [se_index[t] * tiles + t for t in range(tiles)]
    for t in range(tiles):
        rank = sum((keys[other] < keys[t]).astype(jnp.int32) for other in range(tiles) if other != t)
        order[rank] = t
    table[...] = jnp.zeros(table.shape, table.dtype)
    wide[...] = jnp.zeros(wide.shape, wide.dtype)
    found[...] = jnp.zeros(found.shape, found.dtype)
    spread_covariances(roots, grid_scale, comp_base, comp_grid, stack, covar)

    def factoring(pattern):
        return factor_steps(pattern, se_table, covar, prior, upper, inverse, edge, table, bias, tissues)

    def one_tile(step, steps):
        finish_tile(order[jnp.maximum(step - 1, 0)], found, scaled, peak, total)
        scores = score_steps(tissues, packed, table, bias, quad, found)
        for count in range(-(-tissues // GROUP)):
            next(scores, None)
            next(steps, None)
            if count == 2:
                pack_tile(order[jnp.minimum(step + 1, tiles - 1)], effects, wide, ready)
        for _ in scores:
            pass
        for _ in steps:
            pass
        packed[...] = ready[...]

    pack_tile(order[0], effects, wide, packed)
    for _ in factoring(se_index[order[0]]):
        pass

    @pl.loop(0, tiles)
    def _(step):
        later = se_index[order[jnp.minimum(step + 1, tiles - 1)]]
        fresh = se_index[order[step]] != later

        @pl.when(fresh)
        def _():
            one_tile(step, factoring(later))

        @pl.when(jnp.logical_not(fresh))
        def _():
            one_tile(step, iter(()))

    finish_tile(order[tiles - 1], found, scaled, peak, total)


def score_tiles(effects, se_table, se_index, base_root, grid_scale, comp_base, comp_grid, weights):
    tissues, pairs = effects.shape
    bases = base_root.shape[0]
    tiles = se_index.shape[0]
    comps = weights.shape[0]
    width = pairs // tiles
    padded = SUB * (-(-tissues // SUB))
    slot = 16 * (-(-tissues // 16))
    smem = pl.BlockSpec(memory_space=pltpu.SMEM)
    vmem = pl.BlockSpec(memory_space=pltpu.VMEM)
    return pl.pallas_call(
        score_body,
        in_specs=[smem] * 3 + [vmem] * 5,
        out_specs=[vmem] * 3,
        scratch_shapes=[
            pltpu.SMEM((tiles,), jnp.int32),
            pltpu.VMEM((tissues, bases, tissues), jnp.float32),
            pltpu.VMEM((tissues, padded, comps), jnp.float32),
            pltpu.VMEM((tissues, padded, comps), jnp.float32),
            pltpu.VMEM((tissues, padded, comps), jnp.float32),
            pltpu.VMEM((padded, comps), jnp.float32),
            pltpu.VMEM(((tissues + 1) // 2, 4 * slot, 2 * comps), jnp.bfloat16),
            pltpu.VMEM((1, comps), jnp.float32),
            pltpu.VMEM((width, comps), jnp.float32),
            pltpu.VMEM((width, comps), jnp.float32),
            pltpu.VMEM((2 * slot, width), jnp.float32),
            pltpu.VMEM((width, 2 * slot), jnp.bfloat16),
            pltpu.VMEM((width, 2 * slot), jnp.bfloat16),
        ],
        out_shape=[
            jax.ShapeDtypeStruct((comps, pairs), jnp.float32),
            jax.ShapeDtypeStruct((1, pairs), jnp.float32),
            jax.ShapeDtypeStruct((1, pairs), jnp.float32),
        ],
        compiler_params=pltpu.CompilerParams(vmem_limit_bytes=40 * 1024 * 1024),
        name="score_tiles",
    )(se_index, se_table, grid_scale, effects, jnp.transpose(base_root, (1, 0, 2)),
      comp_base[None], comp_grid[None], weights[None])


def combine_body(partners, scaled, peak, total, loglik, factor, log_weights,
                 peak_there, total_there, gathered, send_sem, recv_sem, mass_send, mass_recv):
    comps, pairs = scaled.shape
    groups, places = partners
    width = 512 if pairs % 512 == 0 else pairs
    me_pair, me_comp = lax.axis_index("pairs"), lax.axis_index("comp")
    barrier = pltpu.get_barrier_semaphore()
    for hop in range(1, groups):
        pl.semaphore_signal(barrier, inc=1, device_id=(me_pair, lax.rem(me_comp + hop, groups)), device_id_type=MESH)
    for hop in range(1, places):
        pl.semaphore_signal(barrier, inc=1, device_id=(lax.rem(me_pair + hop, places), me_comp), device_id_type=MESH)
    pl.semaphore_wait(barrier, groups + places - 2)

    copies = []
    for hop in range(1, groups):
        there = (me_pair, lax.rem(me_comp + hop, groups))
        for n, (own, other) in enumerate(((peak, peak_there), (total, total_there))):
            copies.append(pltpu.make_async_remote_copy(
                src_ref=own, dst_ref=other.at[hop - 1],
                send_sem=send_sem.at[2 * hop - 2 + n], recv_sem=recv_sem.at[2 * hop - 2 + n],
                device_id=there, device_id_type=MESH,
            ))
    for copy in copies:
        copy.start()
    for copy in copies:
        copy.wait()
    top = peak[...]
    for hop in range(1, groups):
        top = jnp.maximum(top, peak_there[hop - 1])
    summed = total[...] * jnp.exp(peak[...] - top)
    for hop in range(1, groups):
        summed = summed + total_there[hop - 1] * jnp.exp(peak_there[hop - 1] - top)
    joint = top + jnp.log(summed)
    loglik[...] = joint
    factor[...] = jnp.exp(peak[...] - joint)

    def add_columns(step, acc):
        columns = pl.ds(pl.multiple_of(step * width, width), width)
        posterior = scaled[:, columns] * factor[:, columns]
        for lane in range(0, width, 128):
            acc = acc + posterior[:, lane : lane + 128]
        return acc

    acc = lax.fori_loop(0, pairs // width, add_columns, jnp.zeros((comps, 128), jnp.float32))
    gathered[0] = jnp.sum(acc.T, axis=0, keepdims=True)
    sends = []
    for hop in range(1, places):
        sends.append(pltpu.make_async_remote_copy(
            src_ref=gathered.at[0], dst_ref=gathered.at[hop],
            send_sem=mass_send.at[hop - 1], recv_sem=mass_recv.at[hop - 1],
            device_id=(lax.rem(me_pair + hop, places), me_comp), device_id_type=MESH,
        ))
    for copy in sends:
        copy.start()
    for copy in sends:
        copy.wait()
    masses = gathered[0]
    for hop in range(1, places):
        masses = masses + gathered[hop]
    log_weights[...] = jnp.log((masses + 1.0) / (pairs * places + comps * groups))


def combine(scaled, peak, total):
    comps, pairs = scaled.shape
    groups, places = lax.axis_size("comp"), lax.axis_size("pairs")
    vmem = pl.BlockSpec(memory_space=pltpu.VMEM)

    def body(*refs):
        combine_body((groups, places), *refs)

    return pl.pallas_call(
        body,
        in_specs=[vmem] * 3,
        out_specs=[vmem] * 3,
        out_shape=[
            jax.ShapeDtypeStruct((1, pairs), jnp.float32),
            jax.ShapeDtypeStruct((1, pairs), jnp.float32),
            jax.ShapeDtypeStruct((1, comps), jnp.float32),
        ],
        scratch_shapes=[
            pltpu.VMEM((groups - 1, 1, pairs), jnp.float32),
            pltpu.VMEM((groups - 1, 1, pairs), jnp.float32),
            pltpu.VMEM((places, 1, comps), jnp.float32),
            pltpu.SemaphoreType.DMA((2 * (groups - 1),)),
            pltpu.SemaphoreType.DMA((2 * (groups - 1),)),
            pltpu.SemaphoreType.DMA((places - 1,)),
            pltpu.SemaphoreType.DMA((places - 1,)),
        ],
        compiler_params=pltpu.CompilerParams(
            collective_id=0, has_side_effects=True, vmem_limit_bytes=16 * 1024 * 1024
        ),
        name="combine",
    )(scaled, peak, total)


def per_device(effects, se_table, se_index, base_root, grid_scale, comp_base, comp_grid, weights):
    scaled, peak, total = score_tiles(
        effects, se_table, se_index, base_root, grid_scale, comp_base, comp_grid, weights
    )
    loglik, factor, log_weights = combine(scaled, peak, total)
    return (scaled * factor, log_weights[0], loglik[0])


def solution(mesh):
    placed = (P(None, "pairs"), P(), P("pairs"), P(), P(), P("comp"), P("comp"), P("comp"))
    return jax.shard_map(
        per_device,
        mesh=mesh,
        in_specs=placed,
        out_specs=(P("comp", "pairs"), P("comp"), P("pairs")),
        check_vma=False,
    )
```

```python
import math

import jax
import jax.numpy as jnp
from jax import lax
from jax.experimental import pallas as pl
from jax.experimental.pallas import tpu as pltpu
from jax.sharding import PartitionSpec as P

SUB = 8
GROUP = 4
CHUNKS = 8
VMEM_GRANT = 58 * 1024 * 1024
MESH = pl.DeviceIdType.MESH


def split_terms(value):
    high = value.astype(jnp.bfloat16)
    return high, (value - high.astype(jnp.float32)).astype(jnp.bfloat16)


def put_row(table, row, inv):
    slot = table.shape[1] // 4
    comps = table.shape[2] // 2
    if len(inv) % 2:
        inv = inv + [jnp.zeros((SUB, comps), jnp.float32)]
    high, low = split_terms(jnp.concatenate(inv, axis=0))
    lanes = slice((row % 2) * comps, (row % 2 + 1) * comps)
    height = len(inv) * SUB
    table[row // 2, 0:height, lanes] = high
    table[row // 2, slot : slot + height, lanes] = high
    table[row // 2, 2 * slot : 2 * slot + height, lanes] = low
    table[row // 2, 3 * slot : 3 * slot + height, lanes] = low


def inverse_root(pivot):
    root = lax.rsqrt(pivot)
    return root * (1.5 - 0.5 * pivot * root * root)


def factor_steps(pattern, se_table, covar, prior, upper, inverse, edge, table, bias, tissues):
    constant = 0.5 * tissues * math.log(2.0 * math.pi)
    comps = covar.shape[2]
    border = tissues % SUB == 1
    core = tissues - 1 if border else tissues
    blocks = -(-core // SUB)
    sub_iota = lax.broadcasted_iota(jnp.int32, (SUB, comps), 0)
    half_logdet = jnp.zeros((1, comps), jnp.float32)
    for first in range(0, core, GROUP):
        row_block = first // SUB
        rows = range(first, min(first + GROUP, core))
        system, solved = {}, {}
        for row in rows:
            system[row] = [covar[row, v * SUB : (v + 1) * SUB, :] for v in range(row_block, blocks)]
            on_diag = sub_iota == row % SUB
            deviation = se_table[pattern, row]
            system[row][0] = system[row][0] + jnp.where(on_diag, deviation * deviation, 0.0)
            solved[row] = [jnp.zeros((SUB, comps), jnp.float32) for _ in range(row_block)]
            solved[row].append(jnp.where(on_diag, 1.0, 0.0))
        for col in range(first):
            col_block = col // SUB
            up = [upper[col, v * SUB : (v + 1) * SUB, :] for v in range(row_block, blocks)]
            inv = [inverse[col, v * SUB : (v + 1) * SUB, :] for v in range(col_block + 1)]
            for row in rows:
                mult = upper[col, row : row + 1, :]
                for n, part in enumerate(up):
                    system[row][n] = system[row][n] - mult * part
                for n, part in enumerate(inv):
                    solved[row][n] = solved[row][n] - mult * part
        for row in rows:
            pivot = system[row][0][row % SUB : row % SUB + 1, :]
            root = inverse_root(pivot)
            half_logdet = half_logdet + 0.5 * jnp.log(pivot)
            up = [part * root for part in system[row]]
            inv = [part * root for part in solved[row]]
            for n, part in enumerate(up):
                upper[row, (row_block + n) * SUB : (row_block + n + 1) * SUB, :] = part
            for n, part in enumerate(inv):
                inverse[row, n * SUB : (n + 1) * SUB, :] = part
            for later in rows:
                if later > row:
                    mult = up[0][later % SUB : later % SUB + 1, :]
                    for n, part in enumerate(up):
                        system[later][n] = system[later][n] - mult * part
                    for n, part in enumerate(inv):
                        solved[later][n] = solved[later][n] - mult * part
            put_row(table, row, inv)
            if border:
                terms = [part * covar[core, n * SUB : (n + 1) * SUB, :] for n, part in enumerate(inv)]
                edge[row : row + 1, :] = jnp.sum(sum(terms), axis=0, keepdims=True)
        yield
    if border:
        deviation = se_table[pattern, core]
        pivot = covar[core, core : core + 1, :] + deviation * deviation
        solved = [jnp.zeros((SUB, comps), jnp.float32) for _ in range(blocks)]
        for col in range(core):
            mult = edge[col : col + 1, :]
            pivot = pivot - mult * mult
            for n in range(col // SUB + 1):
                solved[n] = solved[n] - mult * inverse[col, n * SUB : (n + 1) * SUB, :]
        root = inverse_root(pivot)
        half_logdet = half_logdet + 0.5 * jnp.log(pivot)
        solved.append(jnp.where(sub_iota == core % SUB, 1.0, 0.0))
        put_row(table, core, [part * root for part in solved])
        yield
    bias[...] = jnp.log(prior[...]) - half_logdet - constant


def pack_tile(tile, effects, wide, ready):
    tissues = effects.shape[0]
    slot = wide.shape[0] // 2
    width = wide.shape[1]
    values = effects[:, pl.ds(pl.multiple_of(tile * width, width), width)]
    high = values.astype(jnp.bfloat16).astype(jnp.float32)
    wide[0:tissues, :] = high
    wide[slot : slot + tissues, :] = values - high
    ready[...] = wide[...].T.astype(jnp.bfloat16)


def finish_tile(tile, found, scaled, peak, total):
    width = found.shape[0]
    columns = pl.ds(pl.multiple_of(tile * width, width), width)
    values = found[...].T
    top = jnp.max(values, axis=0, keepdims=True)
    shifted = jnp.exp(values - top)
    scaled[:, columns] = shifted
    peak[:, columns] = top
    total[:, columns] = jnp.sum(shifted, axis=0, keepdims=True)


def score_steps(tissues, packed, table, bias, quad, found):
    comps = table.shape[2] // 2
    both = jnp.concatenate([packed[...], packed[...]], axis=1)
    last = table.shape[0] - 1
    for index in range(last + 1):
        if 2 * index + 1 < tissues:
            white = jnp.dot(both, table[index], preferred_element_type=jnp.float32)
            white = white * white
            part = white[:, :comps] + white[:, comps:]
        else:
            white = jnp.dot(both, table[index, :, :comps], preferred_element_type=jnp.float32)
            part = white * white
        if index == 0:
            quad[...] = part
        elif index < last:
            quad[...] += part
        else:
            found[...] = bias[...] - 0.5 * (quad[...] + part)
        if index % (GROUP // 2) == GROUP // 2 - 1:
            yield


def spread_covariances(roots, grid_scale, comp_base, comp_grid, stack, covar):
    tissues, bases = roots.shape[0], roots.shape[1]
    comps = covar.shape[2]
    for base in range(bases):
        root = roots[:, base, :]
        stack[:, base, :] = lax.dot_general(
            root, root, (((1,), (1,)), ((), ())),
            precision=lax.Precision.HIGHEST, preferred_element_type=jnp.float32,
        )
    pick = (lax.broadcasted_iota(jnp.int32, (bases, comps), 0) == comp_base[...]).astype(jnp.float32)
    pick = jnp.concatenate([pick, pick, pick], axis=0).astype(jnp.bfloat16)
    scale = jnp.zeros((1, comps), jnp.float32)
    for grid in range(grid_scale.shape[0]):
        scale = jnp.where(comp_grid[...] == grid, grid_scale[grid], scale)
    scale = scale * scale
    for row in range(tissues):
        value = stack[row]
        high = value.astype(jnp.bfloat16).astype(jnp.float32)
        rest = value - high
        middle = rest.astype(jnp.bfloat16).astype(jnp.float32)
        terms = jnp.concatenate([high, middle, rest - middle], axis=0).astype(jnp.bfloat16)
        spread = lax.dot_general(
            terms, pick, (((0,), (0,)), ((), ())), preferred_element_type=jnp.float32
        )
        covar[row, 0:tissues, :] = spread * scale


def score_body(index_hbm, se_hbm, grid_hbm, effects_hbm, roots_hbm, base_hbm, comp_grid_hbm, prior_hbm,
               scaled_hbm, peak_hbm, total_hbm, scaled, peak, total, sent,
               se_index, se_table, grid_scale, effects, roots, comp_base, comp_grid, prior, arrived,
               order, stack, covar, upper, inverse, edge, table, bias, quad, found, wide, packed, ready):
    tissues = effects.shape[0]
    tiles = se_index.shape[0]
    copies = [
        pltpu.make_async_copy(source, target, arrived.at[n])
        for n, (source, target) in enumerate((
            (roots_hbm, roots), (base_hbm, comp_base), (comp_grid_hbm, comp_grid), (grid_hbm, grid_scale),
            (index_hbm, se_index), (se_hbm, se_table), (prior_hbm, prior), (effects_hbm, effects),
        ))
    ]
    for copy in copies:
        copy.start()
    table[...] = jnp.zeros(table.shape, table.dtype)
    wide[...] = jnp.zeros(wide.shape, wide.dtype)
    found[...] = jnp.zeros(found.shape, found.dtype)
    for copy in copies[:-1]:
        copy.wait()
    keys = [se_index[t] * tiles + t for t in range(tiles)]
    for t in range(tiles):
        rank = sum((keys[other] < keys[t]).astype(jnp.int32) for other in range(tiles) if other != t)
        order[rank] = t
    spread_covariances(roots, grid_scale, comp_base, comp_grid, stack, covar)
    copies[-1].wait()

    def leave(step):
        width = found.shape[0]
        columns = pl.ds(pl.multiple_of(order[step] * width, width), width)
        return pltpu.make_async_copy(scaled.at[:, columns], scaled_hbm.at[:, columns], sent.at[step])

    def factoring(pattern):
        return factor_steps(pattern, se_table, covar, prior, upper, inverse, edge, table, bias, tissues)

    def one_tile(step, steps):
        finish_tile(order[jnp.maximum(step - 1, 0)], found, scaled, peak, total)
        scores = score_steps(tissues, packed, table, bias, quad, found)
        for count in range(-(-tissues // GROUP)):
            next(scores, None)
            next(steps, None)
            if count == 2:
                pack_tile(order[jnp.minimum(step + 1, tiles - 1)], effects, wide, ready)
        for _ in scores:
            pass
        for _ in steps:
            pass
        packed[...] = ready[...]

    pack_tile(order[0], effects, wide, packed)
    for _ in factoring(se_index[order[0]]):
        pass

    @pl.loop(0, tiles)
    def _(step):
        later = se_index[order[jnp.minimum(step + 1, tiles - 1)]]
        fresh = se_index[order[step]] != later

        @pl.when(fresh)
        def _():
            one_tile(step, factoring(later))

        @pl.when(jnp.logical_not(fresh))
        def _():
            one_tile(step, iter(()))

        @pl.when(step > 0)
        def _():
            leave(step - 1).start()

    finish_tile(order[tiles - 1], found, scaled, peak, total)
    last = [
        leave(tiles - 1),
        pltpu.make_async_copy(peak, peak_hbm, sent.at[tiles]),
        pltpu.make_async_copy(total, total_hbm, sent.at[tiles + 1]),
    ]
    for copy in last:
        copy.start()

    @pl.loop(0, tiles - 1)
    def _(step):
        leave(step).wait()

    for copy in last:
        copy.wait()


def score_tiles(effects, se_table, se_index, base_root, grid_scale, comp_base, comp_grid, weights):
    tissues, pairs = effects.shape
    bases = base_root.shape[0]
    tiles = se_index.shape[0]
    comps = weights.shape[0]
    width = pairs // tiles
    padded = SUB * (-(-tissues // SUB))
    slot = 16 * (-(-tissues // 16))
    hbm = pl.BlockSpec(memory_space=pltpu.HBM)
    return pl.pallas_call(
        score_body,
        in_specs=[hbm] * 8,
        out_specs=[hbm] * 3,
        scratch_shapes=[
            pltpu.VMEM((comps, pairs), jnp.float32),
            pltpu.VMEM((1, pairs), jnp.float32),
            pltpu.VMEM((1, pairs), jnp.float32),
            pltpu.SemaphoreType.DMA((tiles + 2,)),
            pltpu.SMEM(se_index.shape, jnp.int32),
            pltpu.SMEM(se_table.shape, jnp.float32),
            pltpu.SMEM(grid_scale.shape, jnp.float32),
            pltpu.VMEM(effects.shape, jnp.float32),
            pltpu.VMEM((tissues, bases, tissues), jnp.float32),
            pltpu.VMEM((1, comps), jnp.int32),
            pltpu.VMEM((1, comps), jnp.int32),
            pltpu.VMEM((1, comps), jnp.float32),
            pltpu.SemaphoreType.DMA((8,)),
            pltpu.SMEM((tiles,), jnp.int32),
            pltpu.VMEM((tissues, bases, tissues), jnp.float32),
            pltpu.VMEM((tissues, padded, comps), jnp.float32),
            pltpu.VMEM((tissues, padded, comps), jnp.float32),
            pltpu.VMEM((tissues, padded, comps), jnp.float32),
            pltpu.VMEM((padded, comps), jnp.float32),
            pltpu.VMEM(((tissues + 1) // 2, 4 * slot, 2 * comps), jnp.bfloat16),
            pltpu.VMEM((1, comps), jnp.float32),
            pltpu.VMEM((width, comps), jnp.float32),
            pltpu.VMEM((width, comps), jnp.float32),
            pltpu.VMEM((2 * slot, width), jnp.float32),
            pltpu.VMEM((width, 2 * slot), jnp.bfloat16),
            pltpu.VMEM((width, 2 * slot), jnp.bfloat16),
        ],
        out_shape=[
            jax.ShapeDtypeStruct((comps, pairs), jnp.float32),
            jax.ShapeDtypeStruct((1, pairs), jnp.float32),
            jax.ShapeDtypeStruct((1, pairs), jnp.float32),
        ],
        compiler_params=pltpu.CompilerParams(vmem_limit_bytes=VMEM_GRANT),
        name="score_tiles",
    )(se_index, se_table, grid_scale, effects, jnp.transpose(base_root, (1, 0, 2)),
      comp_base[None], comp_grid[None], weights[None])


def combine_body(sizes, scaled_hbm, peak_hbm, total_hbm, loglik_hbm, factor_hbm, weights_hbm,
                 scaled, peak, total, loglik, factor, mass, log_weights, peak_there, total_there, gathered,
                 arrived, sent, send_sem, recv_sem, mass_send, mass_recv):
    comps, pairs = scaled.shape
    groups, places = sizes
    width = pairs // CHUNKS
    me_pair, me_comp = lax.axis_index("pairs"), lax.axis_index("comp")
    barrier = pltpu.get_barrier_semaphore()
    partners = [(me_pair, lax.rem(me_comp + hop, groups)) for hop in range(1, groups)]
    peers = [(lax.rem(me_pair + hop, places), me_comp) for hop in range(1, places)]
    for other in peers + partners:
        pl.semaphore_signal(barrier, inc=1, device_id=other, device_id_type=MESH)
    loads = [
        pltpu.make_async_copy(peak_hbm, peak, arrived.at[CHUNKS]),
        pltpu.make_async_copy(total_hbm, total, arrived.at[CHUNKS + 1]),
    ]
    for chunk in range(CHUNKS):
        columns = pl.ds(chunk * width, width)
        loads.append(pltpu.make_async_copy(scaled_hbm.at[:, columns], scaled.at[:, columns], arrived.at[chunk]))
    for copy in loads:
        copy.start()
    for copy in loads[:2]:
        copy.wait()
    pl.semaphore_wait(barrier, groups + places - 2)
    copies = []
    for hop, other in enumerate(partners):
        for n, (own, there) in enumerate(((peak, peak_there), (total, total_there))):
            copies.append(pltpu.make_async_remote_copy(
                src_ref=own, dst_ref=there.at[hop],
                send_sem=send_sem.at[2 * hop + n], recv_sem=recv_sem.at[2 * hop + n],
                device_id=other, device_id_type=MESH,
            ))
    for copy in copies:
        copy.start()
    for copy in loads[2:]:
        copy.wait()
    for copy in copies:
        copy.wait()
    top = peak[...]
    for hop in range(groups - 1):
        top = jnp.maximum(top, peak_there[hop])
    summed = total[...] * jnp.exp(peak[...] - top)
    for hop in range(groups - 1):
        summed = summed + total_there[hop] * jnp.exp(peak_there[hop] - top)
    joint = top + jnp.log(summed)
    loglik[...] = joint
    factor[...] = jnp.exp(peak[...] - joint)

    def add_columns(step, acc):
        columns = pl.ds(pl.multiple_of(step * width, width), width)
        posterior = scaled[:, columns] * factor[:, columns]
        for lane in range(0, width, 128):
            acc = acc + posterior[:, lane : lane + 128]
        return acc

    acc = lax.fori_loop(0, CHUNKS, add_columns, jnp.zeros((comps, 128), jnp.float32))
    mass[...] = jnp.sum(acc.T, axis=0, keepdims=True)
    sends = [
        pltpu.make_async_remote_copy(
            src_ref=mass, dst_ref=gathered.at[hop],
            send_sem=mass_send.at[hop], recv_sem=mass_recv.at[hop],
            device_id=other, device_id_type=MESH,
        )
        for hop, other in enumerate(peers)
    ]
    for copy in sends:
        copy.start()
    leaves = [
        pltpu.make_async_copy(loglik, loglik_hbm, sent.at[0]),
        pltpu.make_async_copy(factor, factor_hbm, sent.at[1]),
        pltpu.make_async_copy(log_weights, weights_hbm, sent.at[2]),
    ]
    for copy in leaves[:2]:
        copy.start()
    for copy in sends:
        copy.wait()
    masses = mass[...]
    for hop in range(places - 1):
        masses = masses + gathered[hop]
    log_weights[...] = jnp.log((masses + 1.0) / (pairs * places + comps * groups))
    leaves[2].start()
    for copy in leaves:
        copy.wait()


def combine(scaled, peak, total):
    comps, pairs = scaled.shape
    groups, places = lax.axis_size("comp"), lax.axis_size("pairs")
    hbm = pl.BlockSpec(memory_space=pltpu.HBM)

    def body(*refs):
        combine_body((groups, places), *refs)

    pair_row, comp_row = (1, pairs), (1, comps)
    return pl.pallas_call(
        body,
        in_specs=[hbm] * 3,
        out_specs=[hbm] * 3,
        out_shape=[
            jax.ShapeDtypeStruct(pair_row, jnp.float32),
            jax.ShapeDtypeStruct(pair_row, jnp.float32),
            jax.ShapeDtypeStruct(comp_row, jnp.float32),
        ],
        scratch_shapes=[
            pltpu.VMEM((comps, pairs), jnp.float32),
            pltpu.VMEM(pair_row, jnp.float32),
            pltpu.VMEM(pair_row, jnp.float32),
            pltpu.VMEM(pair_row, jnp.float32),
            pltpu.VMEM(pair_row, jnp.float32),
            pltpu.VMEM(comp_row, jnp.float32),
            pltpu.VMEM(comp_row, jnp.float32),
            pltpu.VMEM((groups - 1,) + pair_row, jnp.float32),
            pltpu.VMEM((groups - 1,) + pair_row, jnp.float32),
            pltpu.VMEM((places - 1,) + comp_row, jnp.float32),
            pltpu.SemaphoreType.DMA((CHUNKS + 2,)),
            pltpu.SemaphoreType.DMA((3,)),
            pltpu.SemaphoreType.DMA((2 * (groups - 1),)),
            pltpu.SemaphoreType.DMA((2 * (groups - 1),)),
            pltpu.SemaphoreType.DMA((places - 1,)),
            pltpu.SemaphoreType.DMA((places - 1,)),
        ],
        compiler_params=pltpu.CompilerParams(
            collective_id=0, has_side_effects=True, vmem_limit_bytes=VMEM_GRANT
        ),
        name="combine",
    )(scaled, peak, total)


def write_body(scaled_hbm, factor_hbm, loglik_hbm, log_weights_hbm, out, loglik_out, log_weights_out,
               scaled, product, factor, loglik, log_weights, arrived, sent):
    comps, pairs = scaled.shape
    width = pairs // CHUNKS
    places = [pl.ds(chunk * width, width) for chunk in range(CHUNKS)]
    rows = ((factor_hbm, factor), (loglik_hbm, loglik), (log_weights_hbm, log_weights))
    loads = [pltpu.make_async_copy(there, here, arrived.at[n]) for n, (there, here) in enumerate(rows)]
    loads += [
        pltpu.make_async_copy(scaled_hbm.at[:, place], scaled.at[:, place], arrived.at[3 + n])
        for n, place in enumerate(places)
    ]
    for copy in loads:
        copy.start()
    for copy in loads[:3]:
        copy.wait()
    leaves = [
        pltpu.make_async_copy(loglik, loglik_out, sent.at[0]),
        pltpu.make_async_copy(log_weights, log_weights_out, sent.at[1]),
    ]
    for copy in leaves:
        copy.start()
    for n, place in enumerate(places):
        loads[3 + n].wait()
        product[:, place] = scaled[:, place] * factor[:, place]
        leaves.append(pltpu.make_async_copy(product.at[:, place], out.at[:, place], sent.at[2 + n]))
        leaves[-1].start()
    for copy in leaves:
        copy.wait()


def write_out(scaled, factor, loglik, log_weights):
    hbm = pl.BlockSpec(memory_space=pltpu.HBM)
    return pl.pallas_call(
        write_body,
        in_specs=[hbm] * 4,
        out_specs=[hbm] * 3,
        out_shape=[
            jax.ShapeDtypeStruct(scaled.shape, jnp.float32),
            jax.ShapeDtypeStruct(loglik.shape, jnp.float32),
            jax.ShapeDtypeStruct(log_weights.shape, jnp.float32),
        ],
        scratch_shapes=[
            pltpu.VMEM(scaled.shape, jnp.float32),
            pltpu.VMEM(scaled.shape, jnp.float32),
            pltpu.VMEM(factor.shape, jnp.float32),
            pltpu.VMEM(loglik.shape, jnp.float32),
            pltpu.VMEM(log_weights.shape, jnp.float32),
            pltpu.SemaphoreType.DMA((3 + CHUNKS,)),
            pltpu.SemaphoreType.DMA((2 + CHUNKS,)),
        ],
        compiler_params=pltpu.CompilerParams(vmem_limit_bytes=VMEM_GRANT),
        name="write_out",
    )(scaled, factor, loglik, log_weights)


def per_device(effects, se_table, se_index, base_root, grid_scale, comp_base, comp_grid, weights):
    scaled, peak, total = score_tiles(
        effects, se_table, se_index, base_root, grid_scale, comp_base, comp_grid, weights
    )
    loglik, factor, log_weights = combine(scaled, peak, total)
    responsibility, loglik, log_weights = write_out(scaled, factor, loglik, log_weights)
    return (responsibility, log_weights[0], loglik[0])


def solution(mesh):
    placed = (P(None, "pairs"), P(), P("pairs"), P(), P(), P("comp"), P("comp"), P("comp"))
    return jax.shard_map(
        per_device,
        mesh=mesh,
        in_specs=placed,
        out_specs=(P("comp", "pairs"), P("comp"), P("pairs")),
        check_vma=False,
    )
```

```python
import math

import jax
import jax.numpy as jnp
from jax import lax
from jax.experimental import pallas as pl
from jax.experimental.pallas import tpu as pltpu
from jax.sharding import PartitionSpec as P

SUB = 8
GROUP = 4
CHUNKS = 8
VMEM_GRANT = 58 * 1024 * 1024
MESH = pl.DeviceIdType.MESH


def split_terms(value):
    high = value.astype(jnp.bfloat16)
    return high, (value - high.astype(jnp.float32)).astype(jnp.bfloat16)


def put_row(table, row, inv):
    slot = table.shape[1] // 4
    comps = table.shape[2] // 2
    if len(inv) % 2:
        inv = inv + [jnp.zeros((SUB, comps), jnp.float32)]
    high, low = split_terms(jnp.concatenate(inv, axis=0))
    lanes = slice((row % 2) * comps, (row % 2 + 1) * comps)
    height = len(inv) * SUB
    table[row // 2, 0:height, lanes] = high
    table[row // 2, slot : slot + height, lanes] = high
    table[row // 2, 2 * slot : 2 * slot + height, lanes] = low
    table[row // 2, 3 * slot : 3 * slot + height, lanes] = low


def factor_steps(pattern, se_table, covar, prior, upper, inverse, edge, pivots, table, bias, tissues):
    constant = 0.5 * tissues * math.log(2.0 * math.pi)
    comps = covar.shape[2]
    border = tissues % SUB == 1
    core = tissues - 1 if border else tissues
    blocks = -(-core // SUB)
    sub_iota = lax.broadcasted_iota(jnp.int32, (SUB, comps), 0)
    for first in range(0, core, GROUP):
        row_block = first // SUB
        rows = range(first, min(first + GROUP, core))
        system, solved = {}, {}
        for row in rows:
            system[row] = [covar[row, v * SUB : (v + 1) * SUB, :] for v in range(row_block, blocks)]
            on_diag = sub_iota == row % SUB
            deviation = se_table[pattern, row]
            system[row][0] = system[row][0] + jnp.where(on_diag, deviation * deviation, 0.0)
            solved[row] = [jnp.zeros((SUB, comps), jnp.float32) for _ in range(row_block)]
            solved[row].append(jnp.where(on_diag, 1.0, 0.0))
        for col in range(first):
            col_block = col // SUB
            up = [upper[col, v * SUB : (v + 1) * SUB, :] for v in range(row_block, blocks)]
            inv = [inverse[col, v * SUB : (v + 1) * SUB, :] for v in range(col_block + 1)]
            for row in rows:
                mult = upper[col, row : row + 1, :]
                for n, part in enumerate(up):
                    system[row][n] = system[row][n] - mult * part
                for n, part in enumerate(inv):
                    solved[row][n] = solved[row][n] - mult * part
        for row in rows:
            pivot = system[row][0][row % SUB : row % SUB + 1, :]
            root = lax.rsqrt(pivot)
            pivots[row : row + 1, :] = pivot
            up = [part * root for part in system[row]]
            inv = [part * root for part in solved[row]]
            for n, part in enumerate(up):
                upper[row, (row_block + n) * SUB : (row_block + n + 1) * SUB, :] = part
            for n, part in enumerate(inv):
                inverse[row, n * SUB : (n + 1) * SUB, :] = part
            for later in rows:
                if later > row:
                    mult = up[0][later % SUB : later % SUB + 1, :]
                    for n, part in enumerate(up):
                        system[later][n] = system[later][n] - mult * part
                    for n, part in enumerate(inv):
                        solved[later][n] = solved[later][n] - mult * part
            put_row(table, row, inv)
            if border:
                terms = [part * covar[core, n * SUB : (n + 1) * SUB, :] for n, part in enumerate(inv)]
                edge[row * SUB : (row + 1) * SUB, :] = sum(terms)
        yield
    if border:
        deviation = se_table[pattern, core]
        pivot = covar[core, core : core + 1, :] + deviation * deviation
        solved = [jnp.zeros((SUB, comps), jnp.float32) for _ in range(blocks)]
        for block in range(blocks):
            lines = [edge[pl.ds(block * SUB * SUB + n, SUB, stride=SUB), :] for n in range(SUB)]
            edge[core * SUB + block * SUB : core * SUB + (block + 1) * SUB, :] = sum(lines)
        for col in range(core):
            mult = edge[core * SUB + col : core * SUB + col + 1, :]
            pivot = pivot - mult * mult
            for n in range(col // SUB + 1):
                solved[n] = solved[n] - mult * inverse[col, n * SUB : (n + 1) * SUB, :]
        root = lax.rsqrt(pivot)
        pivots[core : core + 1, :] = pivot
        solved.append(jnp.where(sub_iota == core % SUB, 1.0, 0.0))
        put_row(table, core, [part * root for part in solved])
        yield
    logdet = jnp.sum(jnp.log(pivots[...]), axis=0, keepdims=True)
    bias[...] = jnp.log(prior[...]) - 0.5 * logdet - constant


def pack_tile(tile, effects, wide, ready):
    tissues = effects.shape[0]
    slot = wide.shape[0] // 2
    width = wide.shape[1]
    values = effects[:, pl.ds(pl.multiple_of(tile * width, width), width)]
    high = values.astype(jnp.bfloat16).astype(jnp.float32)
    wide[0:tissues, :] = high
    wide[slot : slot + tissues, :] = values - high
    ready[...] = wide[...].T.astype(jnp.bfloat16)


def finish_tile(tile, found, scaled, peak, total):
    width = found.shape[0]
    columns = pl.ds(pl.multiple_of(tile * width, width), width)
    values = found[...].T
    top = jnp.max(values, axis=0, keepdims=True)
    shifted = jnp.exp(values - top)
    scaled[:, columns] = shifted
    peak[:, columns] = top
    total[:, columns] = jnp.sum(shifted, axis=0, keepdims=True)


def score_steps(tissues, packed, table, bias, quad, found):
    comps = table.shape[2] // 2
    both = jnp.concatenate([packed[...], packed[...]], axis=1)
    last = table.shape[0] - 1
    for index in range(last + 1):
        if 2 * index + 1 < tissues:
            white = jnp.dot(both, table[index], preferred_element_type=jnp.float32)
            white = white * white
            part = white[:, :comps] + white[:, comps:]
        else:
            white = jnp.dot(both, table[index, :, :comps], preferred_element_type=jnp.float32)
            part = white * white
        if index == 0:
            quad[...] = part
        elif index < last:
            quad[...] += part
        else:
            found[...] = bias[...] - 0.5 * (quad[...] + part)
        if index % (GROUP // 2) == GROUP // 2 - 1:
            yield


def spread_covariances(roots, grid_scale, comp_base, comp_grid, stack, covar):
    tissues, bases = roots.shape[0], roots.shape[1]
    comps = covar.shape[2]
    for base in range(bases):
        root = roots[:, base, :]
        stack[:, base, :] = lax.dot_general(
            root, root, (((1,), (1,)), ((), ())),
            precision=lax.Precision.HIGHEST, preferred_element_type=jnp.float32,
        )
    pick = (lax.broadcasted_iota(jnp.int32, (bases, comps), 0) == comp_base[...]).astype(jnp.float32)
    pick = jnp.concatenate([pick, pick, pick], axis=0).astype(jnp.bfloat16)
    scale = jnp.zeros((1, comps), jnp.float32)
    for grid in range(grid_scale.shape[0]):
        scale = jnp.where(comp_grid[...] == grid, grid_scale[grid], scale)
    scale = scale * scale
    for row in range(tissues):
        value = stack[row]
        high = value.astype(jnp.bfloat16).astype(jnp.float32)
        rest = value - high
        middle = rest.astype(jnp.bfloat16).astype(jnp.float32)
        terms = jnp.concatenate([high, middle, rest - middle], axis=0).astype(jnp.bfloat16)
        spread = lax.dot_general(
            terms, pick, (((0,), (0,)), ((), ())), preferred_element_type=jnp.float32
        )
        covar[row, 0:tissues, :] = spread * scale


def score_body(index_hbm, se_hbm, grid_hbm, effects_hbm, roots_hbm, base_hbm, comp_grid_hbm, prior_hbm,
               scaled_hbm, peak_hbm, total_hbm, scaled, peak, total, sent,
               se_index, se_table, grid_scale, effects, roots, comp_base, comp_grid, prior, arrived,
               order, stack, covar, upper, inverse, edge, pivots, table, bias, quad, found, wide, packed, ready):
    tissues = effects.shape[0]
    tiles = se_index.shape[0]
    copies = [
        pltpu.make_async_copy(source, target, arrived.at[n])
        for n, (source, target) in enumerate((
            (roots_hbm, roots), (base_hbm, comp_base), (comp_grid_hbm, comp_grid), (grid_hbm, grid_scale),
            (index_hbm, se_index), (se_hbm, se_table), (prior_hbm, prior), (effects_hbm, effects),
        ))
    ]
    for copy in copies:
        copy.start()
    table[...] = jnp.zeros(table.shape, table.dtype)
    wide[...] = jnp.zeros(wide.shape, wide.dtype)
    pivots[...] = jnp.ones(pivots.shape, pivots.dtype)
    found[...] = jnp.zeros(found.shape, found.dtype)
    for copy in copies[:-1]:
        copy.wait()
    keys = [se_index[t] * tiles + t for t in range(tiles)]
    for t in range(tiles):
        rank = sum((keys[other] < keys[t]).astype(jnp.int32) for other in range(tiles) if other != t)
        order[rank] = t
    spread_covariances(roots, grid_scale, comp_base, comp_grid, stack, covar)
    copies[-1].wait()

    def leave(step):
        width = found.shape[0]
        columns = pl.ds(pl.multiple_of(order[step] * width, width), width)
        return pltpu.make_async_copy(scaled.at[:, columns], scaled_hbm.at[:, columns], sent.at[step])

    def factoring(pattern):
        return factor_steps(pattern, se_table, covar, prior, upper, inverse, edge, pivots, table, bias, tissues)

    def one_tile(step, steps):
        finish_tile(order[jnp.maximum(step - 1, 0)], found, scaled, peak, total)
        scores = score_steps(tissues, packed, table, bias, quad, found)
        for count in range(-(-tissues // GROUP)):
            next(scores, None)
            next(steps, None)
            if count == 2:
                pack_tile(order[jnp.minimum(step + 1, tiles - 1)], effects, wide, ready)
        for _ in scores:
            pass
        for _ in steps:
            pass
        packed[...] = ready[...]

    pack_tile(order[0], effects, wide, packed)
    for _ in factoring(se_index[order[0]]):
        pass

    @pl.loop(0, tiles)
    def _(step):
        later = se_index[order[jnp.minimum(step + 1, tiles - 1)]]
        fresh = se_index[order[step]] != later

        @pl.when(fresh)
        def _():
            one_tile(step, factoring(later))

        @pl.when(jnp.logical_not(fresh))
        def _():
            one_tile(step, iter(()))

        @pl.when(step > 0)
        def _():
            leave(step - 1).start()

    finish_tile(order[tiles - 1], found, scaled, peak, total)
    last = [
        leave(tiles - 1),
        pltpu.make_async_copy(peak, peak_hbm, sent.at[tiles]),
        pltpu.make_async_copy(total, total_hbm, sent.at[tiles + 1]),
    ]
    for copy in last:
        copy.start()

    @pl.loop(0, tiles - 1)
    def _(step):
        leave(step).wait()

    for copy in last:
        copy.wait()


def score_tiles(effects, se_table, se_index, base_root, grid_scale, comp_base, comp_grid, weights):
    tissues, pairs = effects.shape
    bases = base_root.shape[0]
    tiles = se_index.shape[0]
    comps = weights.shape[0]
    width = pairs // tiles
    padded = SUB * (-(-tissues // SUB))
    slot = 16 * (-(-tissues // 16))
    hbm = pl.BlockSpec(memory_space=pltpu.HBM)
    return pl.pallas_call(
        score_body,
        in_specs=[hbm] * 8,
        out_specs=[hbm] * 3,
        scratch_shapes=[
            pltpu.VMEM((comps, pairs), jnp.float32),
            pltpu.VMEM((1, pairs), jnp.float32),
            pltpu.VMEM((1, pairs), jnp.float32),
            pltpu.SemaphoreType.DMA((tiles + 2,)),
            pltpu.SMEM(se_index.shape, jnp.int32),
            pltpu.SMEM(se_table.shape, jnp.float32),
            pltpu.SMEM(grid_scale.shape, jnp.float32),
            pltpu.VMEM(effects.shape, jnp.float32),
            pltpu.VMEM((tissues, bases, tissues), jnp.float32),
            pltpu.VMEM((1, comps), jnp.int32),
            pltpu.VMEM((1, comps), jnp.int32),
            pltpu.VMEM((1, comps), jnp.float32),
            pltpu.SemaphoreType.DMA((8,)),
            pltpu.SMEM((tiles,), jnp.int32),
            pltpu.VMEM((tissues, bases, tissues), jnp.float32),
            pltpu.VMEM((tissues, padded, comps), jnp.float32),
            pltpu.VMEM((tissues, padded, comps), jnp.float32),
            pltpu.VMEM((tissues, padded, comps), jnp.float32),
            pltpu.VMEM(((SUB + 1) * padded, comps), jnp.float32),
            pltpu.VMEM((padded, comps), jnp.float32),
            pltpu.VMEM(((tissues + 1) // 2, 4 * slot, 2 * comps), jnp.bfloat16),
            pltpu.VMEM((1, comps), jnp.float32),
            pltpu.VMEM((width, comps), jnp.float32),
            pltpu.VMEM((width, comps), jnp.float32),
            pltpu.VMEM((2 * slot, width), jnp.float32),
            pltpu.VMEM((width, 2 * slot), jnp.bfloat16),
            pltpu.VMEM((width, 2 * slot), jnp.bfloat16),
        ],
        out_shape=[
            jax.ShapeDtypeStruct((comps, pairs), jnp.float32),
            jax.ShapeDtypeStruct((1, pairs), jnp.float32),
            jax.ShapeDtypeStruct((1, pairs), jnp.float32),
        ],
        compiler_params=pltpu.CompilerParams(vmem_limit_bytes=VMEM_GRANT),
        name="score_tiles",
    )(se_index, se_table, grid_scale, effects, jnp.transpose(base_root, (1, 0, 2)),
      comp_base[None], comp_grid[None], weights[None])


def combine_body(sizes, scaled_hbm, peak_hbm, total_hbm, loglik_hbm, factor_hbm, weights_hbm,
                 scaled, peak, total, loglik, factor, mass, log_weights, peak_there, total_there, gathered,
                 arrived, sent, send_sem, recv_sem, mass_send, mass_recv):
    comps, pairs = scaled.shape
    groups, places = sizes
    width = pairs // CHUNKS
    me_pair, me_comp = lax.axis_index("pairs"), lax.axis_index("comp")
    barrier = pltpu.get_barrier_semaphore()
    partners = [(me_pair, lax.rem(me_comp + hop, groups)) for hop in range(1, groups)]
    peers = [(lax.rem(me_pair + hop, places), me_comp) for hop in range(1, places)]
    for other in peers + partners:
        pl.semaphore_signal(barrier, inc=1, device_id=other, device_id_type=MESH)
    loads = [
        pltpu.make_async_copy(peak_hbm, peak, arrived.at[CHUNKS]),
        pltpu.make_async_copy(total_hbm, total, arrived.at[CHUNKS + 1]),
    ]
    for chunk in range(CHUNKS):
        columns = pl.ds(chunk * width, width)
        loads.append(pltpu.make_async_copy(scaled_hbm.at[:, columns], scaled.at[:, columns], arrived.at[chunk]))
    for copy in loads:
        copy.start()
    for copy in loads[:2]:
        copy.wait()
    pl.semaphore_wait(barrier, groups + places - 2)
    copies = []
    for hop, other in enumerate(partners):
        for n, (own, there) in enumerate(((peak, peak_there), (total, total_there))):
            copies.append(pltpu.make_async_remote_copy(
                src_ref=own, dst_ref=there.at[hop],
                send_sem=send_sem.at[2 * hop + n], recv_sem=recv_sem.at[2 * hop + n],
                device_id=other, device_id_type=MESH,
            ))
    for copy in copies:
        copy.start()
    for copy in loads[2:]:
        copy.wait()
    for copy in copies:
        copy.wait()
    top = peak[...]
    for hop in range(groups - 1):
        top = jnp.maximum(top, peak_there[hop])
    summed = total[...] * jnp.exp(peak[...] - top)
    for hop in range(groups - 1):
        summed = summed + total_there[hop] * jnp.exp(peak_there[hop] - top)
    joint = top + jnp.log(summed)
    loglik[...] = joint
    factor[...] = jnp.exp(peak[...] - joint)

    def add_columns(step, acc):
        columns = pl.ds(pl.multiple_of(step * width, width), width)
        posterior = scaled[:, columns] * factor[:, columns]
        for lane in range(0, width, 128):
            acc = acc + posterior[:, lane : lane + 128]
        return acc

    acc = lax.fori_loop(0, CHUNKS, add_columns, jnp.zeros((comps, 128), jnp.float32))
    mass[...] = jnp.sum(acc.T, axis=0, keepdims=True)
    sends = [
        pltpu.make_async_remote_copy(
            src_ref=mass, dst_ref=gathered.at[hop],
            send_sem=mass_send.at[hop], recv_sem=mass_recv.at[hop],
            device_id=other, device_id_type=MESH,
        )
        for hop, other in enumerate(peers)
    ]
    for copy in sends:
        copy.start()
    leaves = [
        pltpu.make_async_copy(loglik, loglik_hbm, sent.at[0]),
        pltpu.make_async_copy(factor, factor_hbm, sent.at[1]),
        pltpu.make_async_copy(log_weights, weights_hbm, sent.at[2]),
    ]
    for copy in leaves[:2]:
        copy.start()
    for copy in sends:
        copy.wait()
    masses = mass[...]
    for hop in range(places - 1):
        masses = masses + gathered[hop]
    log_weights[...] = jnp.log((masses + 1.0) / (pairs * places + comps * groups))
    leaves[2].start()
    for copy in leaves:
        copy.wait()


def combine(scaled, peak, total):
    comps, pairs = scaled.shape
    groups, places = lax.axis_size("comp"), lax.axis_size("pairs")
    hbm = pl.BlockSpec(memory_space=pltpu.HBM)

    def body(*refs):
        combine_body((groups, places), *refs)

    pair_row, comp_row = (1, pairs), (1, comps)
    return pl.pallas_call(
        body,
        in_specs=[hbm] * 3,
        out_specs=[hbm] * 3,
        out_shape=[
            jax.ShapeDtypeStruct(pair_row, jnp.float32),
            jax.ShapeDtypeStruct(pair_row, jnp.float32),
            jax.ShapeDtypeStruct(comp_row, jnp.float32),
        ],
        scratch_shapes=[
            pltpu.VMEM((comps, pairs), jnp.float32),
            pltpu.VMEM(pair_row, jnp.float32),
            pltpu.VMEM(pair_row, jnp.float32),
            pltpu.VMEM(pair_row, jnp.float32),
            pltpu.VMEM(pair_row, jnp.float32),
            pltpu.VMEM(comp_row, jnp.float32),
            pltpu.VMEM(comp_row, jnp.float32),
            pltpu.VMEM((groups - 1,) + pair_row, jnp.float32),
            pltpu.VMEM((groups - 1,) + pair_row, jnp.float32),
            pltpu.VMEM((places - 1,) + comp_row, jnp.float32),
            pltpu.SemaphoreType.DMA((CHUNKS + 2,)),
            pltpu.SemaphoreType.DMA((3,)),
            pltpu.SemaphoreType.DMA((2 * (groups - 1),)),
            pltpu.SemaphoreType.DMA((2 * (groups - 1),)),
            pltpu.SemaphoreType.DMA((places - 1,)),
            pltpu.SemaphoreType.DMA((places - 1,)),
        ],
        compiler_params=pltpu.CompilerParams(
            collective_id=0, has_side_effects=True, vmem_limit_bytes=VMEM_GRANT
        ),
        name="combine",
    )(scaled, peak, total)


def write_body(scaled_hbm, factor_hbm, loglik_hbm, log_weights_hbm, out, loglik_out, log_weights_out,
               scaled, product, factor, loglik, log_weights, arrived, sent):
    comps, pairs = scaled.shape
    width = pairs // CHUNKS
    places = [pl.ds(chunk * width, width) for chunk in range(CHUNKS)]
    rows = ((factor_hbm, factor), (loglik_hbm, loglik), (log_weights_hbm, log_weights))
    loads = [pltpu.make_async_copy(there, here, arrived.at[n]) for n, (there, here) in enumerate(rows)]
    loads += [
        pltpu.make_async_copy(scaled_hbm.at[:, place], scaled.at[:, place], arrived.at[3 + n])
        for n, place in enumerate(places)
    ]
    for copy in loads:
        copy.start()
    for copy in loads[:3]:
        copy.wait()
    leaves = [
        pltpu.make_async_copy(loglik, loglik_out, sent.at[0]),
        pltpu.make_async_copy(log_weights, log_weights_out, sent.at[1]),
    ]
    for copy in leaves:
        copy.start()
    for n, place in enumerate(places):
        loads[3 + n].wait()
        product[:, place] = scaled[:, place] * factor[:, place]
        leaves.append(pltpu.make_async_copy(product.at[:, place], out.at[:, place], sent.at[2 + n]))
        leaves[-1].start()
    for copy in leaves:
        copy.wait()


def write_out(scaled, factor, loglik, log_weights):
    hbm = pl.BlockSpec(memory_space=pltpu.HBM)
    return pl.pallas_call(
        write_body,
        in_specs=[hbm] * 4,
        out_specs=[hbm] * 3,
        out_shape=[
            jax.ShapeDtypeStruct(scaled.shape, jnp.float32),
            jax.ShapeDtypeStruct(loglik.shape, jnp.float32),
            jax.ShapeDtypeStruct(log_weights.shape, jnp.float32),
        ],
        scratch_shapes=[
            pltpu.VMEM(scaled.shape, jnp.float32),
            pltpu.VMEM(scaled.shape, jnp.float32),
            pltpu.VMEM(factor.shape, jnp.float32),
            pltpu.VMEM(loglik.shape, jnp.float32),
            pltpu.VMEM(log_weights.shape, jnp.float32),
            pltpu.SemaphoreType.DMA((3 + CHUNKS,)),
            pltpu.SemaphoreType.DMA((2 + CHUNKS,)),
        ],
        compiler_params=pltpu.CompilerParams(vmem_limit_bytes=VMEM_GRANT),
        name="write_out",
    )(scaled, factor, loglik, log_weights)


def per_device(effects, se_table, se_index, base_root, grid_scale, comp_base, comp_grid, weights):
    scaled, peak, total = score_tiles(
        effects, se_table, se_index, base_root, grid_scale, comp_base, comp_grid, weights
    )
    loglik, factor, log_weights = combine(scaled, peak, total)
    responsibility, loglik, log_weights = write_out(scaled, factor, loglik, log_weights)
    return (responsibility, log_weights[0], loglik[0])


def solution(mesh):
    placed = (P(None, "pairs"), P(), P("pairs"), P(), P(), P("comp"), P("comp"), P("comp"))
    return jax.shard_map(
        per_device,
        mesh=mesh,
        in_specs=placed,
        out_specs=(P("comp", "pairs"), P("comp"), P("pairs")),
        check_vma=False,
    )
```

```python
import math

import jax
import jax.numpy as jnp
from jax import lax
from jax.experimental import pallas as pl
from jax.experimental.pallas import tpu as pltpu
from jax.sharding import PartitionSpec as P

SUB = 8
GROUP = 2
LN2 = math.log(2.0)
LOG2E = 1.0 / LN2
CHUNKS = 8
VMEM_GRANT = 58 * 1024 * 1024
MESH = pl.DeviceIdType.MESH


def split_terms(value):
    high = value.astype(jnp.bfloat16)
    return high, (value - high.astype(jnp.float32)).astype(jnp.bfloat16)


def put_row(table, row, inv):
    slot = table.shape[1] // 4
    comps = table.shape[2] // 2
    if len(inv) % 2:
        inv = inv + [jnp.zeros((SUB, comps), jnp.float32)]
    high, low = split_terms(jnp.concatenate(inv, axis=0))
    lanes = slice((row % 2) * comps, (row % 2 + 1) * comps)
    height = len(inv) * SUB
    table[row // 2, 0:height, lanes] = high
    table[row // 2, slot : slot + height, lanes] = high
    table[row // 2, 2 * slot : 2 * slot + height, lanes] = low
    table[row // 2, 3 * slot : 3 * slot + height, lanes] = low


def factor_steps(pattern, se_table, covar, prior, upper, inverse, edge, pivots, table, bias, tissues):
    constant = 0.5 * tissues * math.log(2.0 * math.pi)
    comps = covar.shape[2]
    border = tissues % SUB == 1
    core = tissues - 1 if border else tissues
    blocks = -(-core // SUB)
    sub_iota = lax.broadcasted_iota(jnp.int32, (SUB, comps), 0)
    for first in range(0, core, GROUP):
        row_block = first // SUB
        rows = range(first, min(first + GROUP, core))
        system, solved = {}, {}
        for row in rows:
            system[row] = [covar[row, v * SUB : (v + 1) * SUB, :] for v in range(row_block, blocks)]
            on_diag = sub_iota == row % SUB
            deviation = se_table[pattern, row]
            system[row][0] = system[row][0] + jnp.where(on_diag, deviation * deviation, 0.0)
            solved[row] = [jnp.zeros((SUB, comps), jnp.float32) for _ in range(row_block)]
            solved[row].append(jnp.where(on_diag, 1.0, 0.0))
        for col in range(first):
            col_block = col // SUB
            up = [upper[col, v * SUB : (v + 1) * SUB, :] for v in range(row_block, blocks)]
            inv = [inverse[col, v * SUB : (v + 1) * SUB, :] for v in range(col_block + 1)]
            for row in rows:
                mult = upper[col, row : row + 1, :]
                for n, part in enumerate(up):
                    system[row][n] = system[row][n] - mult * part
                for n, part in enumerate(inv):
                    solved[row][n] = solved[row][n] - mult * part
        for row in rows:
            pivot = system[row][0][row % SUB : row % SUB + 1, :]
            root = lax.rsqrt(pivot)
            pivots[row : row + 1, :] = pivot
            up = [part * root for part in system[row]]
            inv = [part * root for part in solved[row]]
            for n, part in enumerate(up):
                upper[row, (row_block + n) * SUB : (row_block + n + 1) * SUB, :] = part
            for n, part in enumerate(inv):
                inverse[row, n * SUB : (n + 1) * SUB, :] = part
            for later in rows:
                if later > row:
                    mult = up[0][later % SUB : later % SUB + 1, :]
                    for n, part in enumerate(up):
                        system[later][n] = system[later][n] - mult * part
                    for n, part in enumerate(inv):
                        solved[later][n] = solved[later][n] - mult * part
            put_row(table, row, inv)
            if border:
                terms = [part * covar[core, n * SUB : (n + 1) * SUB, :] for n, part in enumerate(inv)]
                edge[row * SUB : (row + 1) * SUB, :] = sum(terms)
        yield
    if border:
        deviation = se_table[pattern, core]
        pivot = covar[core, core : core + 1, :] + deviation * deviation
        solved = [jnp.zeros((SUB, comps), jnp.float32) for _ in range(blocks)]
        for block in range(blocks):
            lines = [edge[pl.ds(block * SUB * SUB + n, SUB, stride=SUB), :] for n in range(SUB)]
            edge[core * SUB + block * SUB : core * SUB + (block + 1) * SUB, :] = sum(lines)
        for col in range(core):
            mult = edge[core * SUB + col : core * SUB + col + 1, :]
            pivot = pivot - mult * mult
            for n in range(col // SUB + 1):
                solved[n] = solved[n] - mult * inverse[col, n * SUB : (n + 1) * SUB, :]
        root = lax.rsqrt(pivot)
        pivots[core : core + 1, :] = pivot
        solved.append(jnp.where(sub_iota == core % SUB, 1.0, 0.0))
        put_row(table, core, [part * root for part in solved])
        yield
    logdet = jnp.sum(jnp.log(pivots[...]), axis=0, keepdims=True)
    bias[...] = (jnp.log(prior[...]) - 0.5 * logdet - constant) * LOG2E


def pack_tile(tile, effects, wide, ready):
    tissues = effects.shape[0]
    slot = wide.shape[0] // 2
    width = wide.shape[1]
    values = effects[:, pl.ds(pl.multiple_of(tile * width, width), width)]
    high = values.astype(jnp.bfloat16).astype(jnp.float32)
    wide[0:tissues, :] = high
    wide[slot : slot + tissues, :] = values - high
    ready[...] = wide[...].T.astype(jnp.bfloat16)


def finish_tile(tile, found, scaled, peak, total):
    width = found.shape[0]
    columns = pl.ds(pl.multiple_of(tile * width, width), width)
    values = found[...].T
    top = jnp.max(values, axis=0, keepdims=True)
    shifted = jnp.exp2(values - top)
    scaled[:, columns] = shifted
    peak[:, columns] = top * LN2
    total[:, columns] = jnp.sum(shifted, axis=0, keepdims=True)


def score_steps(tissues, packed, table, bias, quad, found):
    comps = table.shape[2] // 2
    both = jnp.concatenate([packed[...], packed[...]], axis=1)
    last = table.shape[0] - 1
    for index in range(last + 1):
        if 2 * index + 1 < tissues:
            white = jnp.dot(both, table[index], preferred_element_type=jnp.float32)
            white = white * white
            part = white[:, :comps] + white[:, comps:]
        else:
            white = jnp.dot(both, table[index, :, :comps], preferred_element_type=jnp.float32)
            part = white * white
        if index == 0:
            quad[...] = part
        elif index < last:
            quad[...] += part
        else:
            found[...] = bias[...] - (0.5 * LOG2E) * (quad[...] + part)
        if index % (GROUP // 2) == GROUP // 2 - 1:
            yield


def spread_covariances(roots, grid_scale, comp_base, comp_grid, stack, covar):
    tissues, bases = roots.shape[0], roots.shape[1]
    comps = covar.shape[2]
    for base in range(bases):
        root = roots[:, base, :]
        stack[:, base, :] = lax.dot_general(
            root, root, (((1,), (1,)), ((), ())),
            precision=lax.Precision.HIGHEST, preferred_element_type=jnp.float32,
        )
    pick = (lax.broadcasted_iota(jnp.int32, (bases, comps), 0) == comp_base[...]).astype(jnp.float32)
    pick = jnp.concatenate([pick, pick, pick], axis=0).astype(jnp.bfloat16)
    scale = jnp.zeros((1, comps), jnp.float32)
    for grid in range(grid_scale.shape[0]):
        scale = jnp.where(comp_grid[...] == grid, grid_scale[grid], scale)
    scale = scale * scale
    for row in range(tissues):
        value = stack[row]
        high = value.astype(jnp.bfloat16).astype(jnp.float32)
        rest = value - high
        middle = rest.astype(jnp.bfloat16).astype(jnp.float32)
        terms = jnp.concatenate([high, middle, rest - middle], axis=0).astype(jnp.bfloat16)
        spread = lax.dot_general(
            terms, pick, (((0,), (0,)), ((), ())), preferred_element_type=jnp.float32
        )
        covar[row, 0:tissues, :] = spread * scale


def score_body(index_hbm, se_hbm, grid_hbm, effects_hbm, roots_hbm, base_hbm, comp_grid_hbm, prior_hbm,
               scaled_hbm, peak_hbm, total_hbm, scaled, peak, total, sent,
               se_index, se_table, grid_scale, effects, roots, comp_base, comp_grid, prior, arrived,
               order, stack, covar, upper, inverse, edge, pivots, table, bias, quad, found, wide, packed, ready):
    tissues = effects.shape[0]
    tiles = se_index.shape[0]
    copies = [
        pltpu.make_async_copy(source, target, arrived.at[n])
        for n, (source, target) in enumerate((
            (roots_hbm, roots), (base_hbm, comp_base), (comp_grid_hbm, comp_grid), (grid_hbm, grid_scale),
            (index_hbm, se_index), (se_hbm, se_table), (prior_hbm, prior), (effects_hbm, effects),
        ))
    ]
    for copy in copies:
        copy.start()
    table[...] = jnp.zeros(table.shape, table.dtype)
    wide[...] = jnp.zeros(wide.shape, wide.dtype)
    pivots[...] = jnp.ones(pivots.shape, pivots.dtype)
    found[...] = jnp.zeros(found.shape, found.dtype)
    for copy in copies[:-1]:
        copy.wait()
    keys = [se_index[t] * tiles + t for t in range(tiles)]
    for t in range(tiles):
        rank = sum((keys[other] < keys[t]).astype(jnp.int32) for other in range(tiles) if other != t)
        order[rank] = t
    spread_covariances(roots, grid_scale, comp_base, comp_grid, stack, covar)
    copies[-1].wait()

    def leave(step):
        width = found.shape[0]
        columns = pl.ds(pl.multiple_of(order[step] * width, width), width)
        return pltpu.make_async_copy(scaled.at[:, columns], scaled_hbm.at[:, columns], sent.at[step])

    def factoring(pattern):
        return factor_steps(pattern, se_table, covar, prior, upper, inverse, edge, pivots, table, bias, tissues)

    def one_tile(step, steps):
        finish_tile(order[jnp.maximum(step - 1, 0)], found, scaled, peak, total)
        scores = score_steps(tissues, packed, table, bias, quad, found)
        for count in range(-(-tissues // GROUP)):
            next(scores, None)
            next(steps, None)
            if count == 2:
                pack_tile(order[jnp.minimum(step + 1, tiles - 1)], effects, wide, ready)
        for _ in scores:
            pass
        for _ in steps:
            pass
        packed[...] = ready[...]

    pack_tile(order[0], effects, wide, packed)
    for _ in factoring(se_index[order[0]]):
        pass

    @pl.loop(0, tiles)
    def _(step):
        later = se_index[order[jnp.minimum(step + 1, tiles - 1)]]
        fresh = se_index[order[step]] != later

        @pl.when(fresh)
        def _():
            one_tile(step, factoring(later))

        @pl.when(jnp.logical_not(fresh))
        def _():
            one_tile(step, iter(()))

        @pl.when(step > 0)
        def _():
            leave(step - 1).start()

    finish_tile(order[tiles - 1], found, scaled, peak, total)
    last = [
        leave(tiles - 1),
        pltpu.make_async_copy(peak, peak_hbm, sent.at[tiles]),
        pltpu.make_async_copy(total, total_hbm, sent.at[tiles + 1]),
    ]
    for copy in last:
        copy.start()

    @pl.loop(0, tiles - 1)
    def _(step):
        leave(step).wait()

    for copy in last:
        copy.wait()


def score_tiles(effects, se_table, se_index, base_root, grid_scale, comp_base, comp_grid, weights):
    tissues, pairs = effects.shape
    bases = base_root.shape[0]
    tiles = se_index.shape[0]
    comps = weights.shape[0]
    width = pairs // tiles
    padded = SUB * (-(-tissues // SUB))
    slot = 16 * (-(-tissues // 16))
    hbm = pl.BlockSpec(memory_space=pltpu.HBM)
    return pl.pallas_call(
        score_body,
        in_specs=[hbm] * 8,
        out_specs=[hbm] * 3,
        scratch_shapes=[
            pltpu.VMEM((comps, pairs), jnp.float32),
            pltpu.VMEM((1, pairs), jnp.float32),
            pltpu.VMEM((1, pairs), jnp.float32),
            pltpu.SemaphoreType.DMA((tiles + 2,)),
            pltpu.SMEM(se_index.shape, jnp.int32),
            pltpu.SMEM(se_table.shape, jnp.float32),
            pltpu.SMEM(grid_scale.shape, jnp.float32),
            pltpu.VMEM(effects.shape, jnp.float32),
            pltpu.VMEM((tissues, bases, tissues), jnp.float32),
            pltpu.VMEM((1, comps), jnp.int32),
            pltpu.VMEM((1, comps), jnp.int32),
            pltpu.VMEM((1, comps), jnp.float32),
            pltpu.SemaphoreType.DMA((8,)),
            pltpu.SMEM((tiles,), jnp.int32),
            pltpu.VMEM((tissues, bases, tissues), jnp.float32),
            pltpu.VMEM((tissues, padded, comps), jnp.float32),
            pltpu.VMEM((tissues, padded, comps), jnp.float32),
            pltpu.VMEM((tissues, padded, comps), jnp.float32),
            pltpu.VMEM(((SUB + 1) * padded, comps), jnp.float32),
            pltpu.VMEM((padded, comps), jnp.float32),
            pltpu.VMEM(((tissues + 1) // 2, 4 * slot, 2 * comps), jnp.bfloat16),
            pltpu.VMEM((1, comps), jnp.float32),
            pltpu.VMEM((width, comps), jnp.float32),
            pltpu.VMEM((width, comps), jnp.float32),
            pltpu.VMEM((2 * slot, width), jnp.float32),
            pltpu.VMEM((width, 2 * slot), jnp.bfloat16),
            pltpu.VMEM((width, 2 * slot), jnp.bfloat16),
        ],
        out_shape=[
            jax.ShapeDtypeStruct((comps, pairs), jnp.float32),
            jax.ShapeDtypeStruct((1, pairs), jnp.float32),
            jax.ShapeDtypeStruct((1, pairs), jnp.float32),
        ],
        compiler_params=pltpu.CompilerParams(vmem_limit_bytes=VMEM_GRANT),
        name="score_tiles",
    )(se_index, se_table, grid_scale, effects, jnp.transpose(base_root, (1, 0, 2)),
      comp_base[None], comp_grid[None], weights[None])


def combine_body(sizes, scaled_hbm, peak_hbm, total_hbm, loglik_hbm, factor_hbm, weights_hbm,
                 scaled, peak, total, loglik, factor, mass, log_weights, peak_there, total_there, gathered,
                 arrived, sent, send_sem, recv_sem, mass_send, mass_recv):
    comps, pairs = scaled.shape
    groups, places = sizes
    width = pairs // CHUNKS
    me_pair, me_comp = lax.axis_index("pairs"), lax.axis_index("comp")
    barrier = pltpu.get_barrier_semaphore()
    partners = [(me_pair, lax.rem(me_comp + hop, groups)) for hop in range(1, groups)]
    peers = [(lax.rem(me_pair + hop, places), me_comp) for hop in range(1, places)]
    for other in peers + partners:
        pl.semaphore_signal(barrier, inc=1, device_id=other, device_id_type=MESH)
    loads = [
        pltpu.make_async_copy(peak_hbm, peak, arrived.at[CHUNKS]),
        pltpu.make_async_copy(total_hbm, total, arrived.at[CHUNKS + 1]),
    ]
    for chunk in range(CHUNKS):
        columns = pl.ds(chunk * width, width)
        loads.append(pltpu.make_async_copy(scaled_hbm.at[:, columns], scaled.at[:, columns], arrived.at[chunk]))
    for copy in loads:
        copy.start()
    for copy in loads[:2]:
        copy.wait()
    pl.semaphore_wait(barrier, groups + places - 2)
    copies = []
    for hop, other in enumerate(partners):
        for n, (own, there) in enumerate(((peak, peak_there), (total, total_there))):
            copies.append(pltpu.make_async_remote_copy(
                src_ref=own, dst_ref=there.at[hop],
                send_sem=send_sem.at[2 * hop + n], recv_sem=recv_sem.at[2 * hop + n],
                device_id=other, device_id_type=MESH,
            ))
    for copy in copies:
        copy.start()
    for copy in loads[2:]:
        copy.wait()
    for copy in copies:
        copy.wait()
    top = peak[...]
    for hop in range(groups - 1):
        top = jnp.maximum(top, peak_there[hop])
    summed = total[...] * jnp.exp(peak[...] - top)
    for hop in range(groups - 1):
        summed = summed + total_there[hop] * jnp.exp(peak_there[hop] - top)
    joint = top + jnp.log(summed)
    loglik[...] = joint
    factor[...] = jnp.exp(peak[...] - joint)

    def add_columns(step, acc):
        columns = pl.ds(pl.multiple_of(step * width, width), width)
        posterior = scaled[:, columns] * factor[:, columns]
        for lane in range(0, width, 128):
            acc = acc + posterior[:, lane : lane + 128]
        return acc

    acc = lax.fori_loop(0, CHUNKS, add_columns, jnp.zeros((comps, 128), jnp.float32))
    mass[...] = jnp.sum(acc.T, axis=0, keepdims=True)
    sends = [
        pltpu.make_async_remote_copy(
            src_ref=mass, dst_ref=gathered.at[hop],
            send_sem=mass_send.at[hop], recv_sem=mass_recv.at[hop],
            device_id=other, device_id_type=MESH,
        )
        for hop, other in enumerate(peers)
    ]
    for copy in sends:
        copy.start()
    leaves = [
        pltpu.make_async_copy(loglik, loglik_hbm, sent.at[0]),
        pltpu.make_async_copy(factor, factor_hbm, sent.at[1]),
        pltpu.make_async_copy(log_weights, weights_hbm, sent.at[2]),
    ]
    for copy in leaves[:2]:
        copy.start()
    for copy in sends:
        copy.wait()
    masses = mass[...]
    for hop in range(places - 1):
        masses = masses + gathered[hop]
    log_weights[...] = jnp.log((masses + 1.0) / (pairs * places + comps * groups))
    leaves[2].start()
    for copy in leaves:
        copy.wait()


def combine(scaled, peak, total):
    comps, pairs = scaled.shape
    groups, places = lax.axis_size("comp"), lax.axis_size("pairs")
    hbm = pl.BlockSpec(memory_space=pltpu.HBM)

    def body(*refs):
        combine_body((groups, places), *refs)

    pair_row, comp_row = (1, pairs), (1, comps)
    return pl.pallas_call(
        body,
        in_specs=[hbm] * 3,
        out_specs=[hbm] * 3,
        out_shape=[
            jax.ShapeDtypeStruct(pair_row, jnp.float32),
            jax.ShapeDtypeStruct(pair_row, jnp.float32),
            jax.ShapeDtypeStruct(comp_row, jnp.float32),
        ],
        scratch_shapes=[
            pltpu.VMEM((comps, pairs), jnp.float32),
            pltpu.VMEM(pair_row, jnp.float32),
            pltpu.VMEM(pair_row, jnp.float32),
            pltpu.VMEM(pair_row, jnp.float32),
            pltpu.VMEM(pair_row, jnp.float32),
            pltpu.VMEM(comp_row, jnp.float32),
            pltpu.VMEM(comp_row, jnp.float32),
            pltpu.VMEM((groups - 1,) + pair_row, jnp.float32),
            pltpu.VMEM((groups - 1,) + pair_row, jnp.float32),
            pltpu.VMEM((places - 1,) + comp_row, jnp.float32),
            pltpu.SemaphoreType.DMA((CHUNKS + 2,)),
            pltpu.SemaphoreType.DMA((3,)),
            pltpu.SemaphoreType.DMA((2 * (groups - 1),)),
            pltpu.SemaphoreType.DMA((2 * (groups - 1),)),
            pltpu.SemaphoreType.DMA((places - 1,)),
            pltpu.SemaphoreType.DMA((places - 1,)),
        ],
        compiler_params=pltpu.CompilerParams(
            collective_id=0, has_side_effects=True, vmem_limit_bytes=VMEM_GRANT
        ),
        name="combine",
    )(scaled, peak, total)


def write_body(scaled_hbm, factor_hbm, loglik_hbm, log_weights_hbm, out, loglik_out, log_weights_out,
               scaled, product, factor, loglik, log_weights, arrived, sent):
    comps, pairs = scaled.shape
    width = pairs // CHUNKS
    places = [pl.ds(chunk * width, width) for chunk in range(CHUNKS)]
    rows = ((factor_hbm, factor), (loglik_hbm, loglik), (log_weights_hbm, log_weights))
    loads = [pltpu.make_async_copy(there, here, arrived.at[n]) for n, (there, here) in enumerate(rows)]
    loads += [
        pltpu.make_async_copy(scaled_hbm.at[:, place], scaled.at[:, place], arrived.at[3 + n])
        for n, place in enumerate(places)
    ]
    for copy in loads:
        copy.start()
    for copy in loads[:3]:
        copy.wait()
    leaves = [
        pltpu.make_async_copy(loglik, loglik_out, sent.at[0]),
        pltpu.make_async_copy(log_weights, log_weights_out, sent.at[1]),
    ]
    for copy in leaves:
        copy.start()
    for n, place in enumerate(places):
        loads[3 + n].wait()
        product[:, place] = scaled[:, place] * factor[:, place]
        leaves.append(pltpu.make_async_copy(product.at[:, place], out.at[:, place], sent.at[2 + n]))
        leaves[-1].start()
    for copy in leaves:
        copy.wait()


def write_out(scaled, factor, loglik, log_weights):
    hbm = pl.BlockSpec(memory_space=pltpu.HBM)
    return pl.pallas_call(
        write_body,
        in_specs=[hbm] * 4,
        out_specs=[hbm] * 3,
        out_shape=[
            jax.ShapeDtypeStruct(scaled.shape, jnp.float32),
            jax.ShapeDtypeStruct(loglik.shape, jnp.float32),
            jax.ShapeDtypeStruct(log_weights.shape, jnp.float32),
        ],
        scratch_shapes=[
            pltpu.VMEM(scaled.shape, jnp.float32),
            pltpu.VMEM(scaled.shape, jnp.float32),
            pltpu.VMEM(factor.shape, jnp.float32),
            pltpu.VMEM(loglik.shape, jnp.float32),
            pltpu.VMEM(log_weights.shape, jnp.float32),
            pltpu.SemaphoreType.DMA((3 + CHUNKS,)),
            pltpu.SemaphoreType.DMA((2 + CHUNKS,)),
        ],
        compiler_params=pltpu.CompilerParams(vmem_limit_bytes=VMEM_GRANT),
        name="write_out",
    )(scaled, factor, loglik, log_weights)


def per_device(effects, se_table, se_index, base_root, grid_scale, comp_base, comp_grid, weights):
    scaled, peak, total = score_tiles(
        effects, se_table, se_index, base_root, grid_scale, comp_base, comp_grid, weights
    )
    loglik, factor, log_weights = combine(scaled, peak, total)
    responsibility, loglik, log_weights = write_out(scaled, factor, loglik, log_weights)
    return (responsibility, log_weights[0], loglik[0])


def solution(mesh):
    placed = (P(None, "pairs"), P(), P("pairs"), P(), P(), P("comp"), P("comp"), P("comp"))
    return jax.shard_map(
        per_device,
        mesh=mesh,
        in_specs=placed,
        out_specs=(P("comp", "pairs"), P("comp"), P("pairs")),
        check_vma=False,
    )
```
